32 devices in a mesh: rep: 1 (over z), dp: 32 (over x, y, core).
Axes of the slice: x: 4, y: 4, z: 1, core: 2. Of those that a mesh axis runs over, the one named last changes fastest.
The devices are a block of a 4x4x8 slice.
Arguments:
- x: bfloat16 [32, 2048, 1280], P(('rep', 'dp'))
- dy: bfloat16 [32, 2048, 1280], P(('rep', 'dp'))
- w_gate: bfloat16 [2, 1280, 4096], replicated
- w_up: bfloat16 [2, 1280, 4096], replicated
- w_down: bfloat16 [2, 4096, 1280], replicated
- m_w_gate: float32 [2, 1280, 4096], P(None, 'dp')
- m_w_up: float32 [2, 1280, 4096], P(None, 'dp')
- m_w_down: float32 [2, 4096, 1280], P(None, 'dp')
- v_w_gate: float32 [2, 1280, 4096], P(None, 'dp')
- v_w_up: float32 [2, 1280, 4096], P(None, 'dp')
- v_w_down: float32 [2, 4096, 1280], P(None, 'dp')
Outputs:
- output 1: bfloat16 [2, 1280, 4096], P('rep')
- output 2: bfloat16 [2, 1280, 4096], P('rep')
- output 3: bfloat16 [2, 4096, 1280], P('rep')
- output 4: float32 [2, 1280, 4096], P('rep', 'dp')
- output 5: float32 [2, 1280, 4096], P('rep', 'dp')
- output 6: float32 [2, 4096, 1280], P('rep', 'dp')
- output 7: float32 [2, 1280, 4096], P('rep', 'dp')
- output 8: float32 [2, 1280, 4096], P('rep', 'dp')
- output 9: float32 [2, 4096, 1280], P('rep', 'dp')
All inputs are finite; a program needn't handle non-finite values.
Results may differ from the reference program's by a relative error of at most 0.022.
Values are sent between devices in bfloat16 or wider.
A program may use at most 768 MiB of HBM per device.

```python
import jax
import jax.numpy as jnp
from jax import lax

SEQUENCES = 32
TOKENS = 2048
D = 1280
FF = 4096
LAYERS = 2
NAMES = ("w_gate", "w_up", "w_down")
SHAPES = {"w_gate": (LAYERS, D, FF), "w_up": (LAYERS, D, FF), "w_down": (LAYERS, FF, D)}


def bump(key, n, height):
    away = (jnp.arange(n, dtype=jnp.int32) - jax.random.randint(key, (), 0, n, jnp.int32)) % n
    return jnp.where(away < n // 8, height, 1.0)


def together(key, own, strength):
    shared = jax.random.normal(key, own.shape[1:], jnp.float32)
    return (own + strength * shared) * lax.rsqrt(1 + strength * strength)


def setup_inputs(seed: int = 0, part: int = 0) -> dict:
    kx, kdy, ka, kb, kz, kf, kh, kl, *keys = jax.random.split(jax.random.key(seed), 8 + 3 * len(NAMES))
    kx, kdy, ka, kb = (jax.random.fold_in(k, part) for k in (kx, kdy, ka, kb))
    kw, km, kv = (keys[i::3] for i in range(3))
    shape = (SEQUENCES, TOKENS, D)
    much_x, much_dy = jax.random.uniform(kz, (2,), jnp.float32, 0.0, 1.0)
    loud = 2.0 ** jax.random.uniform(jax.random.fold_in(kz, 1), (), jnp.float32, -1.0, 2.0)
    layers = 2.0 ** jax.random.uniform(kl, (LAYERS, 1, 1), jnp.float32, -1.0, 1.0)
    x = together(ka, jax.random.normal(kx, shape, jnp.float32), much_x) * bump(kf, D, 4.0)
    dy = together(kb, jax.random.normal(kdy, shape, jnp.float32), much_dy)
    drawn = {"x": x.astype(jnp.bfloat16), "dy": (loud * dy * (SEQUENCES * TOKENS) ** -0.5).astype(jnp.bfloat16)}
    for key, name in zip(kw, NAMES, strict=True):
        w = jax.random.normal(key, SHAPES[name], jnp.float32) * SHAPES[name][1] ** -0.5
        drawn[name] = (w * {"w_gate": 1.0, "w_up": bump(kh, FF, 4.0), "w_down": layers}[name]).astype(jnp.bfloat16)
    for key, name in zip(km, NAMES, strict=True):
        drawn[f"m_{name}"] = 0.1 * jax.random.normal(key, SHAPES[name], jnp.float32)
    for key, name in zip(kv, NAMES, strict=True):
        drawn[f"v_{name}"] = jax.random.uniform(key, SHAPES[name], jnp.float32, 0.005, 0.015)
    return drawn


def matmul(a, w):
    return jnp.dot(a, w, preferred_element_type=jnp.float32).astype(jnp.bfloat16)


def normed(h):
    wide = h.astype(jnp.float32)
    scale = lax.rsqrt(jnp.mean(wide**2, -1, keepdims=True) + 1e-6)
    return (wide * scale).astype(jnp.bfloat16)


def layer(h, w):
    a = normed(h)
    gate = jnp.dot(a, w["w_gate"], preferred_element_type=jnp.float32)
    up = jnp.dot(a, w["w_up"], preferred_element_type=jnp.float32)
    return h + matmul((jax.nn.silu(gate) * up).astype(jnp.bfloat16), w["w_down"])


def adamw(w, m, v, g):
    m = 0.9 * m + 0.1 * g
    v = 0.95 * v + 0.05 * g * g
    step = m * lax.rsqrt(v + 1e-8) + 0.1 * w
    return (w - 0.02 * step).astype(jnp.bfloat16), m, v


def stack(weights, h):
    return lax.scan(lambda h, w: (layer(h, w), None), h, weights)[0]


def reference(x, dy, w_gate, w_up, w_down, m_w_gate, m_w_up, m_w_down, v_w_gate, v_w_up, v_w_down):
    weights = dict(zip(NAMES, (w_gate, w_up, w_down), strict=True))

    def take(so_far, sequence):
        h, by_y = sequence
        _, back = jax.vjp(lambda w: stack(w, h), weights)
        return jax.tree.map(lambda total, term: total + term.astype(jnp.float32), so_far, back(by_y)[0]), None

    none_yet = {name: jnp.zeros(w.shape, jnp.float32) for name, w in weights.items()}
    by_weights, _ = lax.scan(take, none_yet, (x, dy))
    gradients = [by_weights[name].astype(jnp.bfloat16).astype(jnp.float32) for name in NAMES]
    new = [
        adamw(w.astype(jnp.float32), m, v, g)
        for w, m, v, g in zip((w_gate, w_up, w_down), (m_w_gate, m_w_up, m_w_down), (v_w_gate, v_w_up, v_w_down), gradients, strict=True)
    ]
    return tuple(one[which] for which in range(3) for one in new)
```

```python
import math

import jax
import jax.numpy as jnp
from jax import lax
from jax.experimental import pallas as pl
from jax.experimental.pallas import tpu as pltpu
from jax.sharding import PartitionSpec as P

F32, BF = jnp.float32, jnp.bfloat16
VMEM_LIMIT = 63 * 2**20
MESH = pl.DeviceIdType.MESH


def dot(a, b, ca=1, cb=0):
    return lax.dot_general(a, b, (((ca,), (cb,)), ((), ())), preferred_element_type=F32)


def normed(h):
    wide = h.astype(F32)
    scale = lax.rsqrt(jnp.mean(wide * wide, -1, keepdims=True) + 1e-6)
    return (wide * scale).astype(BF)


def whole(shape):
    return pl.BlockSpec(shape, lambda *i: (0,) * len(shape), pipeline_mode=pl.Buffered(1))


def cost(flops, read):
    return pl.CostEstimate(flops=flops, bytes_accessed=read, transcendentals=0)


class Sum:
    def __init__(self, n, r, c, chunks, slots, staged):
        self.side = math.isqrt(n // 2)
        assert self.side == 4 and self.side * self.side * 2 == n
        self.r, self.c, self.chunks, self.slots, self.staged = r, c, chunks, slots, staged

    def scratch(self):
        s, r, c, n = self.slots, self.r, self.c, self.side
        return [
            pltpu.VMEM((s, 2 if self.staged else 1, 2, 2, n, n, r, c), BF),
            pltpu.VMEM((s, 2, 2, n, n, r, c), BF),
            pltpu.VMEM((s, 2, 6, n, r, c), BF),
            pltpu.VMEM((s, 2, 6, n, r, c), BF),
            pltpu.VMEM((s, 2, 2, n, r, c), F32),
            pltpu.VMEM((s, 2, 6, r, c), BF),
            pltpu.VMEM((s, 2, 6, r, c), BF),
            pltpu.SemaphoreType.DMA((s, 3)),
            pltpu.SemaphoreType.DMA((s, 2, 12)),
            pltpu.SemaphoreType.DMA((s, 2, 12)),
        ]

    def bind(self, put, terms, other, o1, i1, t, o2, i2, sem, ssem, rsem, source=None):
        self.put, self.terms, self.other, self.o1, self.i1, self.t, self.o2, self.i2 = put, terms, other, o1, i1, t, o2, i2
        self.sem, self.ssem, self.rsem, self.source = sem, ssem, rsem, source
        me = lax.axis_index("dp")
        self.core = lax.rem(me, 2)
        self.place = (me // (2 * self.side), lax.rem(me // 2, self.side))
        self.partner = me + 1 - 2 * self.core
        return self

    def along(self, axis, d):
        return lax.rem(self.place[axis] + d + self.side, self.side)

    def hop(self, axis, d):
        x, y = (self.along(a, d) if a == axis else self.place[a] for a in (0, 1))
        return (x * self.side + y) * 2 + self.core

    def greet(self):
        barrier = pltpu.get_barrier_semaphore()
        for device in [self.partner] + [self.hop(axis, d) for axis in (0, 1) for d in (1, -1)]:
            pl.semaphore_signal(barrier, inc=1, device_id={"dp": device}, device_id_type=MESH)

    def met(self):
        pl.semaphore_wait(pltpu.get_barrier_semaphore(), 5)

    def slot(self, k):
        return lax.rem(k, self.slots) if not isinstance(k, int) else k % self.slots

    def mine(self):
        return self.core if self.staged else 0

    def across(self, k):
        s = self.slot(k)
        src = self.terms.at[s, 1 - self.core] if self.staged else self.source.at[1 - self.core, k]
        return pltpu.make_async_remote_copy(
            src, self.other.at[s], self.sem.at[s, 1], self.sem.at[s, 2], device_id={"dp": self.partner}, device_id_type=MESH
        )

    def local(self, k):
        s = self.slot(k)
        return pltpu.make_async_copy(self.source.at[self.core, k], self.terms.at[s, 0], self.sem.at[s, 0])

    def message(self, k, o, phase, m):
        s = self.slot(k)
        src, dst = (self.o1, self.i1) if phase == 0 else (self.o2, self.i2)
        i = 6 * phase + m
        return pltpu.make_async_remote_copy(
            src.at[s, o, m],
            dst.at[s, o, m],
            self.ssem.at[s, o, i],
            self.rsem.at[s, o, i],
            device_id={"dp": self.hop(o if phase == 0 else 1 - o, 1 if m % 2 == 0 else -1)},
            device_id_type=MESH,
        )

    def send(self, k, phase, ms):
        for m in ms:
            for o in (0, 1):
                self.message(k, o, phase, m).start()

    def sent(self, k, phase):
        for o in (0, 1):
            for m in range(6):
                self.message(k, o, phase, m).wait_send()

    def reuse(self, k, phase):
        if isinstance(k, int):
            if k >= self.slots:
                self.sent(k - self.slots, phase)
        elif self.chunks > self.slots:
            pl.when(k >= self.slots)(lambda: self.sent(k - self.slots, phase))

    def pair(self, k, o, half, d):
        s, at = self.slot(k), self.along(o, d)
        if o == 0:
            return self.terms[s, self.mine(), o, half, at].astype(F32) + self.other[s, o, half, at].astype(F32)
        return self.terms[s, self.mine(), o, half, :, at].astype(F32) + self.other[s, o, half, :, at].astype(F32)

    OWN = ((2, 0), (2, 1), (1, 1), (-1, 0))
    PASSED = ((0, 1, 0), (1, -1, 1))
    ARRIVED = ((0, 4, 3), (1, 2, 5))

    def event0(self, k):
        s = self.slot(k)
        if not self.staged:
            self.local(k).wait()
        self.across(k).wait_recv()
        self.reuse(k, 0)
        for o in (0, 1):
            for m, (d, half) in enumerate(self.OWN):
                self.o1[s, o, m] = self.pair(k, o, half, d).astype(BF)
        self.send(k, 0, range(4))

    def event1(self, k):
        s = self.slot(k)
        for o in (0, 1):
            for m, d, half in self.PASSED:
                self.message(k, o, 0, m).wait_recv()
                self.o1[s, o, 4 + m] = (self.pair(k, o, half, d) + self.i1[s, o, m].astype(F32)).astype(BF)
        self.send(k, 0, (4, 5))

    def event2(self, k):
        s = self.slot(k)
        self.reuse(k, 1)
        for o in (0, 1):
            for m in (2, 3, 4, 5):
                self.message(k, o, 0, m).wait_recv()
            for half, a, b in self.ARRIVED:
                self.t[s, o, half] = self.pair(k, o, half, 0) + self.i1[s, o, a].astype(F32) + self.i1[s, o, b].astype(F32)
            for m, (d, half) in enumerate(self.OWN):
                self.o2[s, o, m] = self.t[s, o, half, self.along(1 - o, d)].astype(BF)
        self.send(k, 1, range(4))

    def event3(self, k):
        s = self.slot(k)
        for o in (0, 1):
            for m, d, half in self.PASSED:
                self.message(k, o, 1, m).wait_recv()
                self.o2[s, o, 4 + m] = (self.t[s, o, half, self.along(1 - o, d)] + self.i2[s, o, m].astype(F32)).astype(BF)
        self.send(k, 1, (4, 5))

    def event4(self, k):
        s = self.slot(k)
        for o in (0, 1):
            for m in (2, 3, 4, 5):
                self.message(k, o, 1, m).wait_recv()
            for half, a, b in self.ARRIVED:
                total = self.t[s, o, half, self.along(1 - o, 0)] + self.i2[s, o, a].astype(F32) + self.i2[s, o, b].astype(F32)
                self.put(k, o, half, total)

    def finish(self):
        for k in range(self.chunks - min(self.slots, self.chunks), self.chunks):
            self.across(k).wait_send()
            for phase in (0, 1):
                self.sent(k, phase)

    def when(self, k, event):
        pl.when((k >= 0) & (k < self.chunks))(lambda: event(k))


def gate_up(x, wg, wu, layer, bn=256, bm=512):
    t, d = x.shape
    ff = wg.shape[-1]

    def kernel(x, wg, wu, a, hid, g_out, u_out):
        @pl.when(pl.program_id(0) == 0)
        def _():
            for i in range(t // 256):
                rows = pl.ds(i * 256, 256)
                a[rows, :] = normed(x[rows, :])

        for i in range(t // bm):
            rows = pl.ds(i * bm, bm)
            g, u = dot(a[rows, :], wg[...]), dot(a[rows, :], wu[...])
            hid[rows, :] = (g * jax.nn.sigmoid(g) * u).astype(BF)
            g_out[rows, :] = g
            u_out[rows, :] = u

    w = pl.BlockSpec((None, d, bn), lambda j: (layer, 0, j))
    o = pl.BlockSpec((t, bn), lambda j: (0, j))
    return pl.pallas_call(
        kernel,
        grid=(ff // bn,),
        in_specs=[whole((t, d)), w, w],
        out_specs=[whole((t, d)), o, o, o],
        out_shape=[jax.ShapeDtypeStruct((t, d), BF)] + [jax.ShapeDtypeStruct((t, ff), dt) for dt in (BF, F32, F32)],
        compiler_params=pltpu.CompilerParams(vmem_limit_bytes=VMEM_LIMIT),
        cost_estimate=cost(4 * t * d * ff, 12 * t * ff),
        name="gate_up",
    )(x, wg, wu)


def down(hid, wd, h, layer, bm=256):
    t, ff = hid.shape
    d = wd.shape[-1]

    def kernel(hid, wd, h, y_out, a_out):
        y = h[...] + dot(hid[...], wd[...]).astype(BF)
        y_out[...] = y
        a_out[...] = normed(y)

    o = pl.BlockSpec((bm, d), lambda j: (j, 0))
    return pl.pallas_call(
        kernel,
        grid=(t // bm,),
        in_specs=[
            pl.BlockSpec((bm, ff), lambda j: (j, 0)),
            pl.BlockSpec((None, ff, d), lambda j: (layer, 0, 0), pipeline_mode=pl.Buffered(1)),
            o,
        ],
        out_specs=[o, o],
        out_shape=[jax.ShapeDtypeStruct((t, d), BF)] * 2,
        compiler_params=pltpu.CompilerParams(vmem_limit_bytes=VMEM_LIMIT),
        cost_estimate=cost(2 * t * d * ff, 2 * t * ff),
        name="down",
    )(hid, wd, h)


def stream(total, steps, j, compute):
    s = j // 2

    @pl.when(j == 0)
    def _():
        total.greet()

    @pl.when(j < steps)
    def _():
        @pl.when((lax.rem(j, 2) == 0) & (s >= total.slots))
        def _():
            total.across(s - total.slots).wait_send()

        compute()

    @pl.when(j == 0)
    def _():
        total.met()

    @pl.when((lax.rem(j, 2) == 1) & (j < steps))
    def _():
        total.across(s).start()

    @pl.when(lax.rem(j, 2) == 0)
    def _():
        total.when(s - 2, total.event2)
        total.when(s - 1, total.event0)
        total.when(s - 3, total.event4)

    @pl.when(lax.rem(j, 2) == 1)
    def _():
        total.when(s - 1, total.event1)
        total.when(s - 2, total.event3)

    @pl.when(j == steps + 4)
    def _():
        total.finish()


def projections(n, a, cot, wd, layer, cid, wg=None, wu=None, gate=None, up=None, bn=256, bm=512):
    t, d = a.shape
    ff = wd.shape[-2]
    last = wg is not None
    steps = ff // bn
    r = d // n
    total = Sum(n, r, bn, steps // 2, 3, True)
    n_in, n_out = 5, 5 if last else 2

    def kernel(*refs):
        a, cot, wd, p, q = refs[:n_in]
        outs = refs[n_in : n_in + n_out]
        rest = refs[n_in + n_out :]
        sums = outs[-2:]
        at, rest = rest[0], rest[1:]
        if last:
            hid, dg, du = outs[:3]
        else:
            (dg, du), rest = rest[:2], rest[2:]
        j = pl.program_id(0)

        def put(k, o, half, value):
            sums[o][2 * k + half] = value.astype(BF)

        total.bind(put, *rest)

        @pl.when(j == 0)
        def _():
            for i in range(t // bm):
                at[:, pl.ds(i * bm, bm)] = a[pl.ds(i * bm, bm), :].T

        def compute():
            for i in range(t // bm):
                rows = pl.ds(i * bm, bm)
                if last:
                    g, u = dot(a[rows, :], p[...]), dot(a[rows, :], q[...])
                else:
                    g, u = p[rows, :], q[rows, :]
                dh = dot(cot[rows, :], wd[...], 1, 1).astype(BF).astype(F32)
                s = jax.nn.sigmoid(g)
                silu = g * s
                if last:
                    hid[rows, :] = (silu * u).astype(BF)
                du[rows, :] = (dh * silu).astype(BF)
                dg[rows, :] = (dh * u * (s * (1 + g * (1 - s)))).astype(BF)
            slot, half = total.slot(j // 2), lax.rem(j, 2)
            for o, src in ((0, dg), (1, du)):
                grad = dot(at[...], src[...]).astype(BF)
                for b in range(n):
                    x, y, core = b // (2 * total.side), b // 2 % total.side, b % 2
                    total.terms[slot, core, o, half, x, y] = grad[b * r : (b + 1) * r, :]

        stream(total, steps, j, compute)

    def to(f):
        return lambda j: f(jnp.minimum(j, steps - 1))

    o = pl.BlockSpec((t, bn), to(lambda j: (0, j)))
    w = pl.BlockSpec((None, d, bn), to(lambda j: (layer, 0, j)))
    flops = (10 if last else 6) * t * d * ff
    got = pl.pallas_call(
        kernel,
        grid=(steps + 5,),
        in_specs=[whole((t, d)), whole((t, d)), pl.BlockSpec((None, bn, d), to(lambda j: (layer, j, 0)))] + ([w, w] if last else [o, o]),
        out_specs=([o] * 3 if last else []) + [whole((steps, r, bn))] * 2,
        out_shape=([jax.ShapeDtypeStruct((t, ff), BF)] * 3 if last else []) + [jax.ShapeDtypeStruct((steps, r, bn), BF)] * 2,
        scratch_shapes=[pltpu.VMEM((d, t), BF)] + ([] if last else [pltpu.VMEM((t, bn), BF)] * 2) + total.scratch(),
        compiler_params=pltpu.CompilerParams(vmem_limit_bytes=VMEM_LIMIT, collective_id=cid, has_side_effects=True),
        cost_estimate=cost(flops, 10 * t * ff),
        name="projections_last" if last else "projections",
    )(a, cot, wd, *((wg, wu) if last else (gate, up)))
    *rest, sg, su = got
    return rest, [v.transpose(1, 0, 2).reshape(r, ff) for v in (sg, su)]


PR, PC = 16, 640


def d_down(n, hid, dy, bk=512):
    t, ff = hid.shape
    d = dy.shape[-1]
    r = ff // n
    pieces = (r // PR) * (d // PC)
    chips = bk // (2 * r)

    def kernel(hid, dy, out):
        grad = dot(hid[...], dy[...], 0, 0).astype(BF)
        for chip in range(chips):
            for core in (0, 1):
                for p in range(pieces):
                    i, h = p // (d // PC), p % (d // PC)
                    top = (chip * 2 + core) * r + i * PR
                    out[core, p, chip] = grad[top : top + PR, h * PC : (h + 1) * PC]

    shape = (2, pieces, n // 2, PR, PC)
    out = pl.pallas_call(
        kernel,
        grid=(ff // bk,),
        in_specs=[pl.BlockSpec((t, bk), lambda j: (0, j)), whole((t, d))],
        out_specs=pl.BlockSpec((2, pieces, chips, PR, PC), lambda j: (0, 0, j, 0, 0)),
        out_shape=jax.ShapeDtypeStruct(shape, BF),
        compiler_params=pltpu.CompilerParams(vmem_limit_bytes=VMEM_LIMIT),
        cost_estimate=cost(2 * t * d * ff, 2 * t * ff),
        name="d_down",
    )(hid, dy)
    side = math.isqrt(n // 2)
    return out.reshape(2, pieces // 4, 2, 2, side, side, PR, PC)


def unpiece(v, r, d):
    return v.reshape(r // PR, d // PC, PR, PC).transpose(0, 2, 1, 3).reshape(r, d)


def d_in(n, dg, du, wg, wu, h, dy, terms, layer, cid, bm=256):
    t, ff = dg.shape
    d = h.shape[-1]
    steps = t // bm
    chunks = terms.shape[1]
    total = Sum(n, PR, PC, chunks, chunks, False)

    def kernel(dg, du, wg, wu, h, dy, source, out, summed, *scratch):
        j = pl.program_id(0)

        def put(k, o, half, value):
            summed[4 * k + 2 * o + half] = value.astype(BF)

        total.bind(put, *scratch, source=source)

        @pl.when(j == 0)
        def _():
            total.greet()
            total.met()
            for k in range(chunks):
                total.across(k).start()
                total.local(k).start()

        def events(j, when):
            when(j - 2, total.event1)
            when(j - 1, total.event0)
            when(j - 4, total.event3)
            when(j - 3, total.event2)
            when(j - 5, total.event4)

        events(j, total.when)
        da = (dot(dg[...], wg[...], 1, 1).astype(BF) + dot(du[...], wu[...], 1, 1).astype(BF)).astype(F32)
        wide = h[...].astype(F32)
        scale = lax.rsqrt(jnp.mean(wide * wide, -1, keepdims=True) + 1e-6)
        inner = jnp.sum(da * wide, -1, keepdims=True) * (scale * scale * scale) / d
        out[...] = dy[...] + (da * scale - wide * inner).astype(BF)

        @pl.when(j == steps - 1)
        def _():
            for late in range(steps, chunks + 5):
                events(late, lambda k, event: event(k) if 0 <= k < chunks else None)
            total.finish()

    row = pl.BlockSpec((bm, ff), lambda j: (j, 0))
    o = pl.BlockSpec((bm, d), lambda j: (j, 0))
    w = pl.BlockSpec((None, d, ff), lambda j: (layer, 0, 0), pipeline_mode=pl.Buffered(1))
    dh, summed = pl.pallas_call(
        kernel,
        grid=(steps,),
        in_specs=[row, row, w, w, o, o, pl.BlockSpec(memory_space=pl.ANY)],
        out_specs=[o, whole((4 * chunks, PR, PC))],
        out_shape=[jax.ShapeDtypeStruct((t, d), BF), jax.ShapeDtypeStruct((4 * chunks, PR, PC), BF)],
        scratch_shapes=total.scratch(),
        compiler_params=pltpu.CompilerParams(vmem_limit_bytes=VMEM_LIMIT, collective_id=cid, has_side_effects=True),
        cost_estimate=cost(4 * t * d * ff, 4 * t * ff),
        name="d_in",
    )(dg, du, wg, wu, h, dy, terms)
    return dh, unpiece(summed, ff // n, d)


def alone(n, terms, cid):
    chunks = terms.shape[1]
    total = Sum(n, PR, PC, chunks, chunks, False)

    def kernel(source, summed, *scratch):
        def put(k, o, half, value):
            summed[4 * k + 2 * o + half] = value.astype(BF)

        total.bind(put, *scratch, source=source)
        total.greet()
        total.met()
        for k in range(chunks):
            total.across(k).start()
            total.local(k).start()
        for w in range(chunks + 4):
            for lag, event in ((1, total.event1), (0, total.event0), (2, total.event2), (3, total.event3), (4, total.event4)):
                if 0 <= w - lag < chunks:
                    event(w - lag)
        total.finish()

    summed = pl.pallas_call(
        kernel,
        in_specs=[pl.BlockSpec(memory_space=pl.ANY)],
        out_specs=pl.BlockSpec(memory_space=pltpu.VMEM),
        out_shape=jax.ShapeDtypeStruct((4 * chunks, PR, PC), BF),
        scratch_shapes=total.scratch(),
        compiler_params=pltpu.CompilerParams(vmem_limit_bytes=VMEM_LIMIT, collective_id=cid, has_side_effects=True),
        name="sum_alone",
    )(terms)
    return summed


def adamw(w, m, v, g):
    w, g = w.astype(F32), g.astype(F32)
    m = 0.9 * m + 0.1 * g
    v = 0.95 * v + 0.05 * g * g
    step = m * lax.rsqrt(v + 1e-8) + 0.1 * w
    return (w - 0.02 * step).astype(BF), m, v


def put_layer(block, layer, layers, into=None, rows=None):
    r, c = block.shape
    rows = rows or r // 8

    def kernel(block, *refs):
        refs[-1][...] = block[...]

    spec = pl.BlockSpec((rows, c), lambda j: (j, 0))
    more = [] if into is None else [into]
    return pl.pallas_call(
        kernel,
        grid=(r // rows,),
        in_specs=[spec] + [pl.BlockSpec(memory_space=pl.ANY)] * len(more),
        out_specs=pl.BlockSpec((None, rows, c), lambda j: (layer, j, 0)),
        out_shape=jax.ShapeDtypeStruct((layers, r, c), block.dtype),
        input_output_aliases={1: 0} if more else {},
        name="put_layer",
    )(block, *more)


def solution(mesh):
    n = mesh.shape["dp"]

    def step(x, dy, wg, wu, wd, *moments):
        x, dy = x[0], dy[0]
        layers = wg.shape[0]
        me = lax.axis_index("dp")
        ws, ms, vs = (wg, wu, wd), moments[:3], moments[3:]

        def update(i, layer, g):
            rows = ms[i].shape[1]
            w = lax.dynamic_slice_in_dim(ws[i][layer], me * rows, rows, 0)
            w, m, v = adamw(w, ms[i][layer], vs[i][layer], g)
            return lax.all_gather(w, "dp", axis=0, tiled=True), m, v

        a0, hid0, g0, u0 = gate_up(x, wg, wu, 0)
        h1, a1 = down(hid0, wd, x, 0)
        (hid1, dg1, du1), (sg1, su1) = projections(n, a1, dy, wd, 1, 1, wg=wg, wu=wu)
        new = {(0, 1): update(0, 1, sg1), (1, 1): update(1, 1, su1)}
        terms1 = d_down(n, hid1, dy)
        dh, sd1 = d_in(n, dg1, du1, wg, wu, h1, dy, terms1, 1, 2)
        new[2, 1] = update(2, 1, sd1)
        terms0 = d_down(n, hid0, dh)
        sd0 = unpiece(alone(n, terms0, 4), terms0.shape[1] * 4 * PR * PC // wd.shape[-1], wd.shape[-1])
        new[2, 0] = update(2, 0, sd0)
        _, (sg0, su0) = projections(n, a0, dh, wd, 0, 3, gate=g0, up=u0)
        new[0, 0], new[1, 0] = update(0, 0, sg0), update(1, 0, su0)
        weights = [put_layer(new[i, 0][0], 0, layers, put_layer(new[i, 1][0], 1, layers)) for i in range(3)]
        return (*weights, *(jnp.stack([new[i, layer][which] for layer in (0, 1)]) for which in (1, 2) for i in range(3)))

    seq, rows = P(("rep", "dp")), P(None, "dp")
    return jax.shard_map(
        step,
        mesh=mesh,
        in_specs=(seq, seq, P(), P(), P()) + (rows,) * 6,
        out_specs=(P("rep"),) * 3 + (P("rep", "dp"),) * 6,
        check_vma=False,
    )
```

```python
import math

import jax
import jax.numpy as jnp
from jax import lax
from jax.experimental import pallas as pl
from jax.experimental.pallas import tpu as pltpu
from jax.sharding import PartitionSpec as P

F32, BF = jnp.float32, jnp.bfloat16
VMEM_LIMIT = 63 * 2**20
MESH = pl.DeviceIdType.MESH
ANY = pl.BlockSpec(memory_space=pl.ANY)
BOTH = (0, 1)
PR, PC = 16, 640


def dot(a, b, ca=1, cb=0):
    return lax.dot_general(a, b, (((ca,), (cb,)), ((), ())), preferred_element_type=F32)


def normed(h):
    wide = h.astype(F32)
    scale = lax.rsqrt(jnp.mean(wide * wide, -1, keepdims=True) + 1e-6)
    return (wide * scale).astype(BF)


def whole(shape):
    return pl.BlockSpec(shape, lambda *i: (0,) * len(shape), pipeline_mode=pl.Buffered(1))


def cost(flops, read):
    return pl.CostEstimate(flops=flops, bytes_accessed=read, transcendentals=0)


class Torus:
    def __init__(self, n):
        self.side = math.isqrt(n // 2)
        assert self.side == 4 and self.side * self.side * 2 == n

    def locate(self):
        me = lax.axis_index("dp")
        chip, self.core = me // 2, lax.rem(me, 2)
        self.place = (chip // self.side, lax.rem(chip, self.side))
        self.partner = 2 * chip + 1 - self.core

    def along(self, axis, d):
        return lax.rem(self.place[axis] + d + self.side, self.side)

    def hop(self, axis, d):
        x, y = (self.along(a, d) if a == axis else self.place[a] for a in BOTH)
        return (x * self.side + y) * 2 + self.core


class Sum(Torus):
    def __init__(self, n, r, c, chunks, slots, staged):
        super().__init__(n)
        self.r, self.c, self.chunks, self.slots, self.staged = r, c, chunks, slots, staged

    def scratch(self):
        s, r, c, n = self.slots, self.r, self.c, self.side
        two = 2
        return [
            pltpu.VMEM((s, two if self.staged else 1, two, two, n, n, r, c), BF),
            pltpu.VMEM((s, two, two, n, n, r, c), BF),
            *[pltpu.VMEM((s, two, 6, n, r, c), BF)] * two,
            pltpu.VMEM((s, two, two, n, r, c), F32),
            *[pltpu.VMEM((s, two, 6, r, c), BF)] * two,
            pltpu.SemaphoreType.DMA((s, 3)),
            *[pltpu.SemaphoreType.DMA((s, two, 12))] * two,
        ]

    def bind(self, put, terms, other, o1, i1, t, o2, i2, sem, ssem, rsem, source=None):
        self.put, self.terms, self.other, self.o1, self.i1, self.t, self.o2, self.i2 = put, terms, other, o1, i1, t, o2, i2
        self.sem, self.ssem, self.rsem, self.source = sem, ssem, rsem, source
        self.locate()

    def greet(self):
        barrier = pltpu.get_barrier_semaphore()
        for device in [self.partner] + [self.hop(axis, d) for axis in BOTH for d in (1, -1)]:
            pl.semaphore_signal(barrier, inc=1, device_id={"dp": device}, device_id_type=MESH)

    def met(self):
        pl.semaphore_wait(pltpu.get_barrier_semaphore(), 5)

    def slot(self, k):
        return lax.rem(k, self.slots) if not isinstance(k, int) else k % self.slots

    def mine(self):
        return self.core if self.staged else 0

    def across(self, k):
        s = self.slot(k)
        src = self.terms.at[s, 1 - self.core] if self.staged else self.source.at[1 - self.core, k]
        return pltpu.make_async_remote_copy(
            src, self.other.at[s], self.sem.at[s, 1], self.sem.at[s, 2], device_id={"dp": self.partner}, device_id_type=MESH
        )

    def local(self, k):
        s = self.slot(k)
        return pltpu.make_async_copy(self.source.at[self.core, k], self.terms.at[s, 0], self.sem.at[s, 0])

    def message(self, k, o, phase, m):
        s = self.slot(k)
        src, dst = (self.o1, self.i1) if phase == 0 else (self.o2, self.i2)
        i = 6 * phase + m
        return pltpu.make_async_remote_copy(
            src.at[s, o, m],
            dst.at[s, o, m],
            self.ssem.at[s, o, i],
            self.rsem.at[s, o, i],
            device_id={"dp": self.hop(o if phase == 0 else 1 - o, 1 if m % 2 == 0 else -1)},
            device_id_type=MESH,
        )

    def send(self, k, phase, ms):
        for m in ms:
            for o in BOTH:
                self.message(k, o, phase, m).start()

    def sent(self, k, phase):
        for o in BOTH:
            for m in range(6):
                self.message(k, o, phase, m).wait_send()

    def reuse(self, k, phase):
        if isinstance(k, int):
            if k >= self.slots:
                self.sent(k - self.slots, phase)
        elif self.chunks > self.slots:
            pl.when(k >= self.slots)(lambda: self.sent(k - self.slots, phase))

    def pair(self, k, o, half, d):
        s, at = self.slot(k), self.along(o, d)
        if o == 0:
            return self.terms[s, self.mine(), o, half, at].astype(F32) + self.other[s, o, half, at].astype(F32)
        return self.terms[s, self.mine(), o, half, :, at].astype(F32) + self.other[s, o, half, :, at].astype(F32)

    OWN = ((2, 0), (2, 1), (1, 1), (-1, 0))
    PASSED = ((0, 1, 0), (1, -1, 1))
    ARRIVED = ((0, 4, 3), (1, 2, 5))

    def event0(self, k):
        s = self.slot(k)
        if not self.staged:
            self.local(k).wait()
        self.across(k).wait_recv()
        self.reuse(k, 0)
        for o in BOTH:
            for m, (d, half) in enumerate(self.OWN):
                self.o1[s, o, m] = self.pair(k, o, half, d).astype(BF)
        self.send(k, 0, range(4))

    def event1(self, k):
        s = self.slot(k)
        for o in BOTH:
            for m, d, half in self.PASSED:
                self.message(k, o, 0, m).wait_recv()
                self.o1[s, o, 4 + m] = (self.pair(k, o, half, d) + self.i1[s, o, m].astype(F32)).astype(BF)
        self.send(k, 0, (4, 5))

    def event2(self, k):
        s = self.slot(k)
        self.reuse(k, 1)
        for o in BOTH:
            for m in (2, 3, 4, 5):
                self.message(k, o, 0, m).wait_recv()
            for half, a, b in self.ARRIVED:
                self.t[s, o, half] = self.pair(k, o, half, 0) + self.i1[s, o, a].astype(F32) + self.i1[s, o, b].astype(F32)
            for m, (d, half) in enumerate(self.OWN):
                self.o2[s, o, m] = self.t[s, o, half, self.along(1 - o, d)].astype(BF)
        self.send(k, 1, range(4))

    def event3(self, k):
        s = self.slot(k)
        for o in BOTH:
            for m, d, half in self.PASSED:
                self.message(k, o, 1, m).wait_recv()
                self.o2[s, o, 4 + m] = (self.t[s, o, half, self.along(1 - o, d)] + self.i2[s, o, m].astype(F32)).astype(BF)
        self.send(k, 1, (4, 5))

    def event4(self, k):
        s = self.slot(k)
        for o in BOTH:
            for m in (2, 3, 4, 5):
                self.message(k, o, 1, m).wait_recv()
            for half, a, b in self.ARRIVED:
                total = self.t[s, o, half, self.along(1 - o, 0)] + self.i2[s, o, a].astype(F32) + self.i2[s, o, b].astype(F32)
                self.put(k, o, half, total)

    def finish(self):
        for k in range(self.chunks - min(self.slots, self.chunks), self.chunks):
            self.across(k).wait_send()
            for phase in BOTH:
                self.sent(k, phase)

    def when(self, k, event):
        pl.when((k >= 0) & (k < self.chunks))(lambda: event(k))


class Spread(Torus):
    def __init__(self, n, r, c, chunks):
        super().__init__(n)
        self.r, self.c, self.chunks = r, c, chunks

    def piece_shape(self):
        return self.chunks, 2, 2, self.r, self.c

    def scratch(self):
        k = self.chunks
        return [pltpu.SemaphoreType.DMA((k, 2))] + [pltpu.SemaphoreType.DMA((k, 2, 9))] * 2

    def outs(self):
        return [jax.ShapeDtypeStruct((self.chunks, 2, self.side, self.side, 2, self.r, self.c), BF)] * 2

    def bind(self, held, fresh, sem, ssem, rsem):
        self.held, self.fresh, self.sem, self.ssem, self.rsem = held, fresh, sem, ssem, rsem
        self.locate()

    def where(self, o, axis, d, k, half, line):
        at = [self.along(a, d) if a == axis else (slice(None) if line else self.place[a]) for a in BOTH]
        return self.held[o].at[k, half, at[0], at[1], self.core]

    def local(self, k, o):
        return pltpu.make_async_copy(self.fresh.at[k, o], self.where(o, 0, 0, k, slice(None), False), self.sem.at[k, o])

    def message(self, k, o, m):
        axis, to = (1 - o if m < 4 else o), 1 if m % 2 == 0 else -1
        if m == 8:
            src = dst = self.held[o].at[k, :, :, :, self.core]
            device = self.partner
        else:
            device = self.hop(axis, to)
            passed = m % 4 >= 2
            src = dst = self.where(o, axis, -to if passed else 0, k, m % 2 if passed else slice(None), m >= 4)
            if m < 2:
                src = self.fresh.at[k, o]
        return pltpu.make_async_remote_copy(
            src, dst, self.ssem.at[k, o, m], self.rsem.at[k, o, m], device_id={"dp": device}, device_id_type=MESH
        )

    def begin(self, k):
        for o in BOTH:
            self.local(k, o).start()
            for m in BOTH:
                self.message(k, o, m).start()

    def pass1(self, k):
        for m in BOTH:
            for o in BOTH:
                self.message(k, o, m).wait_recv()
                self.message(k, o, m + 2).start()

    def turn(self, k):
        for o in BOTH:
            self.local(k, o).wait()
            for m in (2, 3):
                self.message(k, o, m).wait_recv()
            for m in (4, 5):
                self.message(k, o, m).start()

    def pass2(self, k):
        for m in (4, 5):
            for o in BOTH:
                self.message(k, o, m).wait_recv()
                self.message(k, o, m + 2).start()

    def across(self, k):
        for o in BOTH:
            for m in (6, 7):
                self.message(k, o, m).wait_recv()
            self.message(k, o, 8).start()

    def finish(self):
        @pl.loop(0, self.chunks)
        def _(k):
            for o in BOTH:
                self.message(k, o, 8).wait_recv()
                for m in range(9):
                    self.message(k, o, m).wait_send()


def gate_up(x, wg, wu, layer, bn=256, bm=512):
    t, d = x.shape
    ff = wg.shape[-1]

    def kernel(x, wg, wu, a, hid, g_out, u_out):
        @pl.when(pl.program_id(0) == 0)
        def _():
            @pl.loop(0, t // bn)
            def _(i):
                rows = pl.ds(pl.multiple_of(i * bn, bn), bn)
                a[rows, :] = normed(x[rows, :])

        @pl.loop(0, t // (2 * bm))
        def _(i):
            for half in BOTH:
                rows = pl.ds(pl.multiple_of((2 * i + half) * bm, bm), bm)
                g, u = dot(a[rows, :], wg[...]), dot(a[rows, :], wu[...])
                hid[rows, :] = (g * jax.nn.sigmoid(g) * u).astype(BF)
                g_out[rows, :] = g
                u_out[rows, :] = u

    w = pl.BlockSpec((None, d, bn), lambda j: (layer, 0, j))
    o = pl.BlockSpec((t, bn), lambda j: (0, j))
    return pl.pallas_call(
        kernel,
        grid=(ff // bn,),
        in_specs=[whole((t, d)), w, w],
        out_specs=[whole((t, d)), o, o, o],
        out_shape=[jax.ShapeDtypeStruct((t, d), BF)] + [jax.ShapeDtypeStruct((t, ff), dt) for dt in (BF, F32, F32)],
        compiler_params=pltpu.CompilerParams(vmem_limit_bytes=VMEM_LIMIT),
        cost_estimate=cost(4 * t * d * ff, 12 * t * ff),
        name="gate_up",
    )(x, wg, wu)


def down(hid, wd, h, layer, bm=256):
    t, ff = hid.shape
    d = wd.shape[-1]

    def kernel(hid, wd, h, y_out, a_out):
        y = h[...] + dot(hid[...], wd[...]).astype(BF)
        y_out[...] = y
        a_out[...] = normed(y)

    o = pl.BlockSpec((bm, d), lambda j: (j, 0))
    return pl.pallas_call(
        kernel,
        grid=(t // bm,),
        in_specs=[
            pl.BlockSpec((bm, ff), lambda j: (j, 0)),
            pl.BlockSpec((None, ff, d), lambda j: (layer, 0, 0), pipeline_mode=pl.Buffered(1)),
            o,
        ],
        out_specs=[o, o],
        out_shape=[jax.ShapeDtypeStruct((t, d), BF)] * 2,
        compiler_params=pltpu.CompilerParams(vmem_limit_bytes=VMEM_LIMIT),
        cost_estimate=cost(2 * t * d * ff, 2 * t * ff),
        name="down",
    )(hid, wd, h)


class Step:
    def __init__(self, w, m, v, layer):
        self.arrays, self.layer, self.shape = (w, m, v), layer, m.shape[1:]

    def specs(self):
        one = whole(self.shape)
        of_all = pl.BlockSpec((None, *self.shape), lambda *i: (self.layer, 0, 0), pipeline_mode=pl.Buffered(1))
        return [one, of_all, of_all], [one] * 2

    def outs(self):
        return [jax.ShapeDtypeStruct(self.shape, F32)] * 2


def adamw(refs, rows, columns, total):
    w, m, v, new_m, new_v = refs
    at = (rows, columns)
    g = total.astype(BF).astype(F32)
    wide = w[at].astype(F32)
    mm = 0.9 * m[at] + 0.1 * g
    vv = 0.95 * v[at] + 0.05 * g * g
    step = mm * lax.rsqrt(vv + 1e-8) + 0.1 * wide
    new_m[at] = mm
    new_v[at] = vv
    return (wide - 0.02 * step).astype(BF)


def stream(total, spread, steps, j, compute):
    s = j // 2
    even = lax.rem(j, 2) == 0

    pl.when(j == 0)(total.greet)

    @pl.when(even & (s >= total.slots) & (j < steps))
    def _():
        total.across(s - total.slots).wait_send()

    compute()
    pl.when(j == 0)(total.met)

    @pl.when(~even & (j < steps))
    def _():
        total.across(s).start()

    @pl.when(even)
    def _():
        total.when(s - 2, total.event2)
        total.when(s - 1, total.event0)
        total.when(s - 3, total.event4)
        total.when(s - 4, spread.turn)
        total.when(s - 5, spread.across)

    @pl.when(~even)
    def _():
        total.when(s - 1, total.event1)
        total.when(s - 2, total.event3)
        total.when(s - 3, spread.pass1)
        total.when(s - 4, spread.pass2)

    @pl.when(j == steps + 8)
    def _():
        total.finish()
        spread.finish()


def clamp(steps, f):
    return lambda j: f(jnp.minimum(j, steps - 1))


def transposed(at, a, bm=512):
    @pl.loop(0, a.shape[0] // bm)
    def _(i):
        tokens = pl.ds(pl.multiple_of(i * bm, bm), bm)
        at[:, tokens] = a[tokens, :].T


def terms_shape(n, ff, d):
    return 2, (ff // n // PR) * (d // PC), n // 2, PR, PC


def put_terms(out, grad, r):
    across = grad.shape[1] // PC
    for chip in range(grad.shape[0] // (2 * r)):
        for core in BOTH:
            for p in range((r // PR) * across):
                i, h = p // across, p % across
                top = (chip * 2 + core) * r + i * PR
                out[core, p, chip] = grad[top : top + PR, h * PC : (h + 1) * PC]


def gradients(n, a, updates, cid, dg=None, du=None, cot=None, ws=None, layer=None, bn=256, bm=512, late=9):
    t, d = a.shape
    last = ws is not None
    ff = (ws[0] if last else dg).shape[-1]
    steps = ff // bn
    r = d // n
    total = Sum(n, r, bn, steps // 2, 3, True)
    spread = Spread(n, r, bn, total.chunks)
    n_in = 5 if last else 3
    n_out = 3 if last else 0

    def kernel(*refs):
        refs = list(refs)

        def take(count):
            got = refs[:count]
            del refs[:count]
            return got

        ins, before = take(n_in), take(6)
        outs, after, held, (at,) = take(n_out), take(4), take(2), take(1)
        if last:
            a, cot, wg, wu, wd = ins
            dg, du, terms = outs
            (hid,) = take(1)
        else:
            a, dg, du = ins
        spread.bind(held, *take(4))
        j = pl.program_id(0)

        def put(k, o, half, value):
            columns = pl.ds(pl.multiple_of((2 * k + half) * bn, bn), bn)
            new = adamw(before[3 * o : 3 * o + 3] + after[2 * o : 2 * o + 2], slice(None), columns, value)
            spread.fresh[k, o, half] = new
            if o == half == 1:
                spread.begin(k)

        total.bind(put, *refs)
        pl.when(j == 0)(lambda: transposed(at, a))

        def main():
            if last:
                for i in range(t // bm):
                    rows = pl.ds(i * bm, bm)
                    g, u = dot(a[rows, :], wg[...]), dot(a[rows, :], wu[...])
                    dh = dot(cot[rows, :], wd[...], 1, 1).astype(BF).astype(F32)
                    s = jax.nn.sigmoid(g)
                    silu = g * s
                    hid[lax.rem(j, late + 1), rows, :] = (silu * u).astype(BF)
                    du[rows, :] = (dh * silu).astype(BF)
                    dg[rows, :] = (dh * u * (s * (1 + g * (1 - s)))).astype(BF)
            slot, half = total.slot(j // 2), lax.rem(j, 2)

            def rows_of(count, x0, top):
                for o, src in ((0, dg), (1, du)):
                    grad = dot(at[pl.ds(top, d * count // total.side), :], src[...]).astype(BF)
                    for b in range(n * count // total.side):
                        x, y, core = b // (2 * total.side), b // 2 % total.side, b % 2
                        total.terms[slot, core, o, half, x0 + x, y] = grad[b * r : (b + 1) * r, :]

            if last:
                rows_of(total.side, 0, 0)
            else:
                pl.loop(0, total.side)(lambda x: rows_of(1, x, pl.multiple_of(x * (d // total.side), d // total.side)))

        def compute():
            pl.when(j < steps)(main)
            if last:

                @pl.when((j >= late) & (j < steps + late))
                def _():
                    put_terms(terms, dot(hid[lax.rem(j - late, late + 1)], cot[...], 0, 0).astype(BF), ff // n)

        stream(total, spread, steps, j, compute)

    tile = pl.BlockSpec((t, bn), clamp(steps, lambda j: (0, j)))
    in_specs, out_specs, out_shape, args = [whole((t, d))], [], [], [a]
    scratch = [pltpu.VMEM((d, t), BF)]
    if last:
        w = pl.BlockSpec((None, d, bn), clamp(steps, lambda j: (layer, 0, j)))
        in_specs += [whole((t, d)), w, w, pl.BlockSpec((None, bn, d), clamp(steps, lambda j: (layer, j, 0)))]
        args += [cot, *ws]
        two, pieces, chips, *piece = terms_shape(n, ff, d)
        behind = clamp(steps, lambda j: (0, 0, j, 0, 0))
        out_specs = [tile, tile, pl.BlockSpec((two, pieces, bn * n // (2 * ff), *piece), lambda j: behind(jnp.maximum(j - late, 0)))]
        out_shape = [jax.ShapeDtypeStruct((t, ff), BF)] * 2 + [jax.ShapeDtypeStruct((two, pieces, chips, *piece), BF)]
        scratch += [pltpu.VMEM((late + 1, t, bn), BF)]
    else:
        in_specs += [tile, tile]
        args += [dg, du]
    for u in updates:
        into, out = u.specs()
        in_specs, out_specs, out_shape, args = in_specs + into, out_specs + out, out_shape + u.outs(), args + list(u.arrays)
    scratch += [pltpu.VMEM(spread.piece_shape(), BF)]
    out_specs, out_shape, scratch = out_specs + [ANY] * 2, out_shape + spread.outs(), scratch + spread.scratch()
    got = pl.pallas_call(
        kernel,
        grid=(steps + 9,),
        in_specs=in_specs,
        out_specs=out_specs,
        out_shape=out_shape,
        scratch_shapes=scratch + total.scratch(),
        compiler_params=pltpu.CompilerParams(vmem_limit_bytes=VMEM_LIMIT, collective_id=cid, has_side_effects=True),
        cost_estimate=cost((12 if last else 4) * t * d * ff, 10 * t * ff),
        name="gradients_last" if last else "gradients",
    )(*args)
    mg, vg, mu, vu, wg, wu = got[n_out:]
    return got[:n_out], (wg, mg, vg), (wu, mu, vu)


def chunked(n, terms):
    side = math.isqrt(n // 2)
    return terms.reshape(2, terms.shape[1] // 4, 2, 2, side, side, PR, PC)


def place(out, pieces, r):
    for p in range(pieces.shape[0]):
        for b in range(pieces.shape[1]):
            out[pl.ds(b * r, r), pl.ds(p * pieces.shape[3], pieces.shape[3])] = pieces[p, b]


def d_down(n, hid, dy, held, layer, layers, bk=512):
    t, ff = hid.shape
    d = dy.shape[-1]
    steps = ff // bk
    held = [h.reshape(-1, n, *h.shape[-2:]) for h in held]
    r, c = held[0].shape[-2:]
    per = held[0].shape[0] // steps

    def kernel(hid, dy, hg, hu, out, og, ou):
        put_terms(out, dot(hid[...], dy[...], 0, 0).astype(BF), ff // n)
        place(og, hg, r)
        place(ou, hu, r)

    two, pieces, chips, *piece = terms_shape(n, ff, d)
    h = pl.BlockSpec((per, n, r, c), lambda j: (j, 0, 0, 0))
    o = pl.BlockSpec((None, d, per * c), lambda j: (layer, 0, j))
    return pl.pallas_call(
        kernel,
        grid=(steps,),
        in_specs=[pl.BlockSpec((t, bk), lambda j: (0, j)), whole((t, d)), h, h],
        out_specs=[pl.BlockSpec((two, pieces, bk * n // (2 * ff), *piece), lambda j: (0, 0, j, 0, 0)), o, o],
        out_shape=[jax.ShapeDtypeStruct((two, pieces, chips, *piece), BF)] + [jax.ShapeDtypeStruct((layers, d, ff), BF)] * 2,
        compiler_params=pltpu.CompilerParams(vmem_limit_bytes=VMEM_LIMIT),
        cost_estimate=cost(2 * t * d * ff, 2 * t * ff),
        name="d_down",
    )(hid, dy, *held)


def beside(n, terms, update, cid, steps, compute, args, in_specs, out_specs, out_shape, due, extra, flops, name):
    terms = chunked(n, terms)
    chunks = terms.shape[1]
    total = Sum(n, PR, PC, chunks, chunks, False)
    n_in, n_out = len(in_specs), len(out_specs)

    def kernel(*refs):
        ins, before, source = refs[:n_in], refs[n_in : n_in + 3], refs[n_in + 3]
        refs = refs[n_in + 4 :]
        outs, (new, *after), scratch = refs[:n_out], refs[n_out : n_out + 3], refs[n_out + 3 :]
        j = pl.program_id(0)

        def put(k, o, half, value):
            rows = pl.ds(pl.multiple_of((2 * k + o) * PR, PR), PR)
            columns = slice(half * PC, (half + 1) * PC)
            new[rows, columns] = adamw((*before, *after), rows, columns, value)

        total.bind(put, *scratch, source=source)

        @pl.when(j == 0)
        def _():
            total.greet()
            total.met()
            for k in range(chunks):
                total.across(k).start()
                total.local(k).start()

        for event, k, fits in due(j):
            pl.when(fits & (k >= 0) & (k < chunks))(lambda event=event, k=k: getattr(total, event)(k))

        pl.when(j < steps)(lambda: compute(*ins, *outs))
        pl.when(j == steps + extra - 1)(total.finish)

    into, out = update.specs()
    got = pl.pallas_call(
        kernel,
        grid=(steps + extra,),
        in_specs=in_specs + into + [ANY],
        out_specs=out_specs + out[:1] + out,
        out_shape=out_shape + [jax.ShapeDtypeStruct(update.shape, BF)] + update.outs(),
        scratch_shapes=total.scratch(),
        compiler_params=pltpu.CompilerParams(vmem_limit_bytes=VMEM_LIMIT, collective_id=cid, has_side_effects=True),
        cost_estimate=cost(flops, 1),
        name=name,
    )(*args, *update.arrays, terms)
    return got[:n_out], got[n_out:]


def d_in(n, dg, du, wg, wu, h, dy, layer, terms, update, cid, bm=256):
    t, ff = dg.shape
    d = h.shape[-1]
    steps = t // bm

    def compute(dg, du, wg, wu, h, dy, out):
        da = (dot(dg[...], wg[...], 1, 1).astype(BF) + dot(du[...], wu[...], 1, 1).astype(BF)).astype(F32)
        wide = h[...].astype(F32)
        scale = lax.rsqrt(jnp.mean(wide * wide, -1, keepdims=True) + 1e-6)
        inner = jnp.sum(da * wide, -1, keepdims=True) * (scale * scale * scale) / d
        out[...] = dy[...] + (da * scale - wide * inner).astype(BF)

    def due(j):
        return [(f"event{e}", j - lag, j >= 0) for e, lag in ((1, 2), (0, 1), (3, 4), (2, 3), (4, 5))]

    row = pl.BlockSpec((bm, ff), clamp(steps, lambda j: (j, 0)))
    o = pl.BlockSpec((bm, d), clamp(steps, lambda j: (j, 0)))
    w = pl.BlockSpec((None, d, ff), lambda j: (layer, 0, 0), pipeline_mode=pl.Buffered(1))
    (dh,), new = beside(
        n, terms, update, cid, steps, compute, (dg, du, wg, wu, h, dy), [row, row, w, w, o, o], [o],
        [jax.ShapeDtypeStruct((t, d), BF)], due, 1, 4 * t * d * ff, "d_in",
    )
    return dh, new


def d_projections(n, dh, gate, up, wd, layer, terms, update, cid, bn=256, bm=256):
    t, d = dh.shape
    ff = gate.shape[-1]
    steps = ff // bn

    def compute(dh, g, u, wd, dg, du):
        @pl.loop(0, t // bm)
        def _(i):
            rows = pl.ds(pl.multiple_of(i * bm, bm), bm)
            by_hid = dot(dh[rows, :], wd[...], 1, 1).astype(BF).astype(F32)
            gt = g[rows, :]
            s = jax.nn.sigmoid(gt)
            du[rows, :] = (by_hid * (gt * s)).astype(BF)
            dg[rows, :] = (by_hid * u[rows, :] * (s * (1 + gt * (1 - s)))).astype(BF)

    def due(j):
        return [(f"event{e}", (j - first) // 3, (j >= first) & (lax.rem(j - first + 3, 3) == 0)) for e, first in ((1, 3), (0, 1), (3, 7), (2, 5), (4, 9))]

    tile = pl.BlockSpec((t, bn), clamp(steps, lambda j: (0, j)))
    return beside(
        n, terms, update, cid, steps, compute, (dh, gate, up, wd),
        [whole((t, d)), tile, tile, pl.BlockSpec((None, bn, d), clamp(steps, lambda j: (layer, j, 0)))], [tile, tile],
        [jax.ShapeDtypeStruct((t, ff), BF)] * 2, due, 3, 2 * t * d * ff, "d_projections",
    )


def finish(n, held, downs, into, moments, layer, layers, steps=8):
    held = [h.reshape(-1, n, *h.shape[-2:]) for h in held]
    r, c = held[0].shape[-2:]
    per = held[0].shape[0] // steps
    _, rd, d = downs[0].shape
    owners, n_down, n_m, two = n // steps, len(downs), len(moments), len(into)

    def kernel(*refs):
        hg, hu, *refs = refs
        ds, ms, outs = refs[:n_down], refs[n_down : n_down + n_m], refs[n_down + n_m + two :]
        og, ou, od, *om = outs

        @pl.loop(0, n)
        def _(b):
            rows = pl.ds(pl.multiple_of(b * r, 8), r)
            for out, src in ((og, hg), (ou, hu)):
                for p in range(per):
                    out[rows, p * c : (p + 1) * c] = src[p, b]

        @pl.loop(0, owners)
        def _(b):
            for i, src in enumerate(ds):
                od[i, pl.ds(pl.multiple_of(b * rd, rd), rd), :] = src[b]

        @pl.when(pl.program_id(0) == 0)
        def _():
            for i, src in enumerate(ms):
                om[i // layers][i % layers] = src[...]

    h = pl.BlockSpec((per, n, r, c), lambda j: (j, 0, 0, 0))
    o = pl.BlockSpec((None, n * r, per * c), lambda j: (layer, 0, j))
    b = pl.BlockSpec((owners, rd, d), lambda j: (j, 0, 0))
    stacks = [(layers, *m.shape) for m in moments[::layers]]
    return pl.pallas_call(
        kernel,
        grid=(steps,),
        in_specs=[h, h] + [b] * n_down + [whole(m.shape) for m in moments] + [ANY] * two,
        out_specs=[o, o, pl.BlockSpec((layers, owners * rd, d), lambda j: (0, j, 0))] + [whole(x) for x in stacks],
        out_shape=[jax.ShapeDtypeStruct(i.shape, BF) for i in into]
        + [jax.ShapeDtypeStruct((layers, n * rd, d), BF)]
        + [jax.ShapeDtypeStruct(x, F32) for x in stacks],
        input_output_aliases={two + n_down + n_m + i: i for i in BOTH},
        compiler_params=pltpu.CompilerParams(vmem_limit_bytes=VMEM_LIMIT),
        name="finish",
    )(*held, *downs, *moments, *into)


def solution(mesh):
    n = mesh.shape["dp"]

    def step(x, dy, wg, wu, wd, *moments):
        x, dy = x[0], dy[0]
        layers = wg.shape[0]
        me = lax.axis_index("dp")
        ws, ms, vs = (wg, wu, wd), moments[:3], moments[3:]

        def block(i, layer):
            rows, columns = ms[i].shape[1:]
            own = lax.dynamic_slice(ws[i], (layer, me * rows, 0), (1, rows, columns))[0]
            return Step(own, ms[i], vs[i], layer)

        def gather(block):
            return lax.all_gather(block, "dp", axis=0, tiled=False)

        a0, hid0, g0, u0 = gate_up(x, wg, wu, 0)
        h1, a1 = down(hid0, wd, x, 0)
        (dg1, du1, terms1), new_g1, new_u1 = gradients(n, a1, (block(0, 1), block(1, 1)), 1, cot=dy, ws=ws, layer=1)
        dh, new_d1 = d_in(n, dg1, du1, wg, wu, h1, dy, 1, terms1, block(2, 1), 2)
        all_d1 = gather(new_d1[0])
        terms0, *into = d_down(n, hid0, dh, (new_g1[0], new_u1[0]), 1, layers)
        (dg0, du0), new_d0 = d_projections(n, dh, g0, u0, wd, 0, terms0, block(2, 0), 3)
        dg0, all_d1 = lax.optimization_barrier((dg0, all_d1))
        all_d0 = gather(new_d0[0])
        _, new_g0, new_u0 = gradients(n, a0, (block(0, 0), block(1, 0)), 4, dg=dg0, du=du0)
        new = ((new_g0, new_g1), (new_u0, new_u1), (new_d0, new_d1))
        moments = [one[which] for which in (1, 2) for of in new for one in of]
        return tuple(finish(n, (new_g0[0], new_u0[0]), (all_d0, all_d1), into, moments, 0, layers))

    seq, rows = P(("rep", "dp")), P(None, "dp")
    return jax.shard_map(
        step,
        mesh=mesh,
        in_specs=(seq, seq, P(), P(), P()) + (rows,) * 6,
        out_specs=(P("rep"),) * 3 + (P("rep", "dp"),) * 6,
        check_vma=False,
    )
```
